128 devices in a mesh: row: 16 (over x, z_lo, core), col: 8 (over y, z_hi).
Axes of the slice: x: 4, y: 4, z: 4 (z_hi: 2, z_lo: 2; z = z_hi * 2 + z_lo), core: 2. Of those that a mesh axis runs over, the one named last changes fastest.
Arguments:
- schur_tail: float32 [1024, 1024], P(('row', 'col')), as said below
- coupling: float32 [1024, 16384], P(None, 'row'), may hold values from -4 to 4
- ks_lead: float32 [16384, 4096], P('row', 'col'), may hold values from -0.046875 to 0.046875
- ks_tail: float32 [1024, 4096], P('row', 'col'), may hold values from -0.046875 to 0.046875
- inv_mask: int32 [8, 136], replicated, may hold values 0 or 1
- ks_mask: int32 [136, 32], replicated, may hold values 0 or 1
Outputs:
- projected: float32 [1024, 4096], P('row', 'col')
The draws below stay inside these ranges and needn't reach their ends.
Inputs may be any that keep to these rules, and one draw needn't show every extreme that they name: `schur_tail`: symmetric and positive definite, with diagonal entries between about 1 and 32.
All inputs are finite; a program needn't handle non-finite values.
Results may differ from the reference program's by a relative error of at most 0.00009.
Values sent between devices are 32-bit elements; how exact they have to be, the bound alone decides.
No kernel may reach another device: no remote copies, remote signals or barrier semaphores. Data moves between devices by JAX's collectives and lax.ppermute only.
A program may use at most 128 MiB of HBM per device.

```python
import math
import jax
import jax.numpy as jnp
from jax import lax

NL = 16384
BLK = 128
NC = 4096
K = 1024
N = 17408


def draw_schur_tail(key, part):
    key_one = jax.random.fold_in(key, 0)
    key_two = jax.random.fold_in(key, 1)
    key_four = jax.random.fold_in(key, 3)
    entries = jax.random.normal(key_one, (K, K), jnp.float32) * (0.8 / math.sqrt(2.0 * K))
    symmetric = (entries + entries.T) * 0.5
    diagonal_part = jax.random.uniform(key_two, (K,), jnp.float32, 1.0, 2.0)
    vector = jax.random.uniform(key_four, (K,), jnp.float32, 0.5, 1.0)
    matrix = symmetric + jnp.diag(diagonal_part) + 0.02 * vector[:, None] * vector[None, :]
    return matrix


def set_ends(drawn, rng, least, high):
    extent = drawn.shape
    spot = [jax.random.randint(jax.random.fold_in(rng, axis), (), 0, extent[axis]) for axis in range(len(extent))]
    drawn = drawn.at[tuple(spot)].set(least)
    longest = extent.index(max(extent))
    spot[longest] = (spot[longest] + 1) % extent[longest]
    return drawn.at[tuple(spot)].set(high)


def block_levels(key, dims, cuts, least, high):
    gain = 1.0
    for position, blocks in cuts:
        steps = jax.random.uniform(jax.random.fold_in(jax.random.fold_in(key, 6), position), (blocks,), jnp.float32, least / len(cuts), high / len(cuts))
        gain = gain * jnp.repeat(jnp.exp(steps), dims[position] // blocks).reshape((-1,) + (1,) * (len(dims) - 1 - position))
    return gain


def centred(rng, extent, deviation, most, cuts=(), held_as=jnp.bfloat16):
    result = deviation * jax.random.normal(rng, extent, jnp.float32)
    if cuts:
        result = result * block_levels(rng, extent, cuts, -0.22, 0.18)
    return jnp.clip(result, -most, most).astype(held_as)


def setup_inputs(seed: int = 0) -> dict:
    streams_of = jax.random.split(jax.random.key(seed), 7)
    return {
        "schur_tail": draw_schur_tail(jax.random.fold_in(streams_of[6], 71), 0),
        "coupling": centred(streams_of[1], (K, NL), 0.5, 4.0, ((1, 16),), jnp.float32),
        "ks_lead": centred(streams_of[2], (NL, NC), (NL + K) ** -0.5, 0.046875, ((0, 16), (1, 8)), jnp.float32),
        "ks_tail": centred(streams_of[3], (K, NC), (NL + K) ** -0.5, 0.046875, ((0, 16), (1, 8)), jnp.float32),
        "inv_mask": set_ends((jax.random.randint(streams_of[4], (K // BLK, N // BLK), 0, 2) < 1).astype(jnp.int32), jax.random.fold_in(streams_of[4], 1), 0, 1),
        "ks_mask": set_ends((jax.random.randint(streams_of[5], (N // BLK, NC // BLK), 0, 2) < 1).astype(jnp.int32), jax.random.fold_in(streams_of[5], 1), 0, 1),
    }


def expand(block_mask):
    widened = jnp.repeat(block_mask.astype(jnp.float32), BLK, axis=0)
    return jnp.repeat(widened, BLK, axis=1)

def reference(schur_tail, coupling, ks_lead, ks_tail, inv_mask, ks_mask):
    factor = jnp.linalg.cholesky(schur_tail)
    identity = jnp.eye(K, dtype=jnp.float32)
    tail_inverse = jax.scipy.linalg.solve_triangular(factor, identity, lower=True)
    lead_block = -jnp.dot(tail_inverse.astype(jnp.float32), coupling.astype(jnp.float32), precision=lax.Precision.HIGHEST, preferred_element_type=jnp.float32)
    inverse_rows = jnp.concatenate([lead_block, tail_inverse], axis=1) * expand(inv_mask)
    kohn_sham = jnp.concatenate([ks_lead, ks_tail], axis=0) * expand(ks_mask)
    return jnp.dot(inverse_rows.astype(jnp.float32), kohn_sham.astype(jnp.float32), precision=lax.Precision.HIGHEST, preferred_element_type=jnp.float32)
```

```python
import jax
import jax.numpy as jnp
from jax import lax
from jax.experimental import pallas as pl
from jax.experimental.pallas import tpu as pltpu
from jax.sharding import Mesh
from jax.sharding import PartitionSpec as P

BLK = 128
ROW = ("row_0", "row_1", "row_2")
COL = ("col_0", "col_1")
ROW_COL = ROW + COL
CHIPS = ("row_0", "row_1", "col_0", "col_1")
F32 = jnp.float32
BF16 = jnp.bfloat16
SENT = 5
HIGHEST = lax.Precision.HIGHEST


def dot_full(a, b):
    return jnp.dot(a, b, precision=HIGHEST, preferred_element_type=F32)


def dot_left_t(a, b):
    dims = (((0,), (0,)), ((), ()))
    return lax.dot_general(a, b, dims, precision=HIGHEST, preferred_element_type=F32)


def dot_bf16(a, b):
    return jnp.dot(a, b, preferred_element_type=F32)


def halves(x):
    high = x.astype(BF16)
    return high, (x - high.astype(F32)).astype(BF16)


def dot_three(a, b_high, b_low):
    high, low = halves(a)
    return dot_bf16(high, b_high) + (dot_bf16(high, b_low) + dot_bf16(low, b_high))


def factor_panels(rows, sub, lane):
    groups = len(rows)
    for t in range(groups):

        def columns(g):
            return [
                jnp.broadcast_to(rows[g][:, 8 * t + m : 8 * t + m + 1], (8, BLK)) for m in range(8)
            ]

        pivot = columns(t)
        below = {g: columns(g) for g in range(t + 1, groups)}
        here = (lane >= 8 * t) & (lane < 8 * t + 8)
        full = jnp.where(here, jnp.where(lane - 8 * t == sub, 1.0, 0.0), rows[t])
        result = full
        scale = jnp.ones((8, BLK), F32)
        for k in range(8):
            root = lax.rsqrt(jnp.broadcast_to(pivot[k][k : k + 1, :], (8, BLK)))
            factor = jnp.where(sub != k, pivot[k] * root, 0.0)
            line = jnp.broadcast_to(full[k : k + 1, :], (8, BLK)) * root
            for m in range(k + 1, 8):
                pivot[m] = pivot[m] - factor * (
                    jnp.broadcast_to(pivot[m][k : k + 1, :], (8, BLK)) * root
                )
            full = full - factor * line
            result = jnp.where(sub == k, line, result)
            scale = jnp.where(sub == k, root * root, scale)
        rows[t] = result
        if t + 1 < groups:
            full = full * scale
            lines = [jnp.broadcast_to(full[k : k + 1, :], (8, BLK)) for k in range(8)]
            for g in range(t + 1, groups):
                terms = [below[g][k] * lines[k] for k in range(8)]
                while len(terms) > 1:
                    terms = [a + b for a, b in zip(terms[::2], terms[1::2])]
                rows[g] = jnp.where(here, 0.0, rows[g]) - terms[0]
        yield


def kernel(
    where_ref, inv_mask, ks_mask, mine_ref, other_ref, coupling_hbm, lead_hbm, tail_hbm,
    out_ref,
    m_ref, coupling_ref, lead_ref, tail_ref, ch_ref, cl_ref, kh_ref, kl_ref, th_ref, tl_ref, sem,
):
    size = m_ref.shape[0]
    count = size // BLK
    row, col, core = where_ref[0], where_ref[1], where_ref[2]
    copies = [
        pltpu.make_async_copy(coupling_hbm, coupling_ref, sem.at[0]),
        pltpu.make_async_copy(lead_hbm, lead_ref, sem.at[1]),
        pltpu.make_async_copy(tail_hbm, tail_ref, sem.at[2]),
    ]
    for copy in copies:
        copy.start()
    sub = lax.broadcasted_iota(jnp.int32, (8, BLK), 0)
    lane = lax.broadcasted_iota(jnp.int32, (8, BLK), 1)

    def at(i):
        return slice(i * BLK, (i + 1) * BLK)

    for ref, part in ((mine_ref, core), (other_ref, 1 - core)):
        for b in range(count):
            direct = min(SENT, count - b) * BLK
            m_ref[pl.ds(b * BLK + part * 64, 64), b * BLK : b * BLK + direct] = ref[b, :, :direct]
            for o in range(count - b, SENT - 1):
                c = b + o - count
                m_ref[pl.ds(b * BLK + part * 64, 64), at(c)] = ref[b, :, at(o)]
    for c in range(count):
        for b in range(c + SENT, count):
            m_ref[at(c), at(b)] = m_ref[at(b), at(c)].T

    def prepare():
        for copy in copies:
            copy.wait()
        for k in range(count):
            ch_ref[at(k), :], cl_ref[at(k), :] = halves(coupling_ref[at(k), :])
            yield
        for k in range(count):
            for n in range(lead_ref.shape[1] // BLK):
                keep = ks_mask[row * count + k, col * 4 + n].astype(F32)
                kh_ref[at(k), at(n)], kl_ref[at(k), at(n)] = halves(lead_ref[at(k), at(n)] * keep)
            yield
        th_ref[...] = jnp.zeros(th_ref.shape, BF16)
        tl_ref[...] = jnp.zeros(tl_ref.shape, BF16)
        lead_blocks = ks_mask.shape[0] - count
        for n in range(lead_ref.shape[1] // BLK):
            keep = ks_mask[lead_blocks + row // 2, col * 4 + n].astype(F32)
            high, low = halves(tail_ref[:, at(n)] * keep)
            th_ref[pl.ds(core * 64, 64), at(n)] = high
            tl_ref[pl.ds(core * 64, 64), at(n)] = low
        yield

    def trailing(j, rows):
        for i in rows:
            left = m_ref[at(j), at(i)]
            m_ref[at(i), i * BLK :] -= dot_left_t(left, m_ref[at(j), i * BLK :])
            if j > 0:
                m_ref[at(i), : j * BLK] -= dot_left_t(left, m_ref[at(j), : j * BLK])
            m_ref[at(i), at(j)] = -dot_left_t(left, m_ref[at(j), at(j)])
            yield

    def project(i):
        high, low = halves(m_ref[at(i), : (i + 1) * BLK])
        depth = slice(0, (i + 1) * BLK)
        total = None
        for k in range(0, count, 2):
            wide = slice(k * BLK, (k + 2) * BLK)
            lead = dot_bf16(high, ch_ref[depth, wide]) + (
                dot_bf16(high, cl_ref[depth, wide]) + dot_bf16(low, ch_ref[depth, wide])
            )
            keep = [inv_mask[i, row * count + k + q].astype(F32) for q in range(2)]
            lead = jnp.concatenate([lead[:, :BLK] * keep[0], lead[:, BLK:] * keep[1]], axis=1)
            part = dot_three(lead, kh_ref[wide, :], kl_ref[wide, :])
            total = part if total is None else total + part
            yield
        mine = m_ref[at(i), pl.ds(pl.multiple_of(row // 2 * BLK, BLK), BLK)]
        keep = inv_mask[i, inv_mask.shape[1] - count + row // 2]
        mine = jnp.where((keep != 0) & (row // 2 <= i), mine, 0.0)
        out_ref[at(i), :] = dot_three(mine, th_ref[...], tl_ref[...]) - total
        yield

    fillers = [prepare()]
    for j in range(count):
        rows = [m_ref[j * BLK + 8 * g : j * BLK + 8 * g + 8, at(j)] for g in range(16)]
        for step in factor_panels(rows, sub, lane):
            for _ in range(2):
                while fillers:
                    try:
                        next(fillers[0])
                        break
                    except StopIteration:
                        fillers.pop(0)
        while fillers:
            for _ in fillers.pop(0):
                pass
        p = jnp.concatenate([jnp.where(lane <= sub + 8 * g, rows[g], 0.0) for g in range(16)], axis=0)
        m_ref[at(j), at(j)] = p
        if j + 1 < count:
            m_ref[at(j), (j + 1) * BLK :] = dot_full(p, m_ref[at(j), (j + 1) * BLK :])
            left = m_ref[at(j), at(j + 1)]
            m_ref[at(j + 1), at(j + 1)] -= dot_left_t(left, left)
        if j > 0:
            m_ref[at(j), : j * BLK] = dot_full(p, m_ref[at(j), : j * BLK])

        def rest(j):
            if j + 1 < count:
                left = m_ref[at(j), at(j + 1)]
                if j + 2 < count:
                    m_ref[at(j + 1), (j + 2) * BLK :] -= dot_left_t(left, m_ref[at(j), (j + 2) * BLK :])
                if j > 0:
                    m_ref[at(j + 1), : j * BLK] -= dot_left_t(left, m_ref[at(j), : j * BLK])
                m_ref[at(j + 1), at(j)] = -dot_left_t(left, m_ref[at(j), at(j)])
                yield

        fillers = [rest(j), trailing(j, range(j + 2, count)), project(j)]
    while fillers:
        for _ in fillers.pop(0):
            pass


def projected_part(place, inv_mask, ks_mask, mine, other, coupling, ks_lead, ks_tail):
    size = coupling.shape[0]
    lead, width = ks_lead.shape
    vmem = pl.BlockSpec(memory_space=pltpu.VMEM)
    smem = pl.BlockSpec(memory_space=pltpu.SMEM)
    hbm = pl.BlockSpec(memory_space=pl.ANY)
    return pl.pallas_call(
        kernel,
        out_shape=jax.ShapeDtypeStruct((size, width), F32),
        in_specs=[smem, smem, smem, vmem, vmem, hbm, hbm, hbm],
        out_specs=vmem,
        scratch_shapes=[
            pltpu.VMEM((size, size), F32),
            pltpu.VMEM(coupling.shape, F32),
            pltpu.VMEM(ks_lead.shape, F32),
            pltpu.VMEM(ks_tail.shape, F32),
            pltpu.VMEM(coupling.shape, BF16),
            pltpu.VMEM(coupling.shape, BF16),
            pltpu.VMEM(ks_lead.shape, BF16),
            pltpu.VMEM(ks_lead.shape, BF16),
            pltpu.VMEM((BLK, width), BF16),
            pltpu.VMEM((BLK, width), BF16),
            pltpu.SemaphoreType.DMA((3,)),
        ],
        compiler_params=pltpu.CompilerParams(vmem_limit_bytes=48 * 1024 * 1024),
        name="project",
    )(place, inv_mask, ks_mask, mine, other, coupling, ks_lead, ks_tail)


def swap_half(x, axis):
    half = x.shape[0] // 2
    index = lax.axis_index(axis)
    kept = lax.dynamic_slice_in_dim(x, index * half, half, 0)
    sent = lax.dynamic_slice_in_dim(x, (1 - index) * half, half, 0)
    return kept + lax.ppermute(sent, axis, [(0, 1), (1, 0)])


def per_device(schur_tail, coupling, ks_lead, ks_tail, inv_mask, ks_mask):
    row_index = lax.axis_index(ROW)
    col_index = lax.axis_index(COL)
    core_index = lax.axis_index("row_2")
    twice = jnp.concatenate([schur_tail, schur_tail[:, : SENT * BLK - BLK]], axis=1)
    strip = lax.dynamic_slice_in_dim(twice, row_index // 2 * BLK, SENT * BLK, 1)
    chips = 1
    for axis in CHIPS:
        chips *= lax.axis_size(axis)
    copies = jnp.broadcast_to(strip[None], (chips,) + strip.shape)
    mine = lax.all_to_all(copies, CHIPS, split_axis=0, concat_axis=0, tiled=True)
    mine = mine.reshape(-1, BLK // 2, SENT * BLK)
    other = lax.ppermute(mine, "row_2", [(0, 1), (1, 0)])
    place = jnp.stack([row_index, col_index, core_index]).astype(jnp.int32)
    part = projected_part(place, inv_mask, ks_mask, mine, other, coupling, ks_lead, ks_tail)
    part = part.reshape(4, 2, 2, 64, -1)
    core = lax.axis_index("row_2")
    kept = lax.dynamic_index_in_dim(part, core, 2, keepdims=False)
    sent = lax.dynamic_index_in_dim(part, 1 - core, 2, keepdims=False)
    part = kept + lax.ppermute(sent, "row_2", [(0, 1), (1, 0)])
    z = lax.axis_index("row_1")
    kept = lax.dynamic_index_in_dim(part, z, 1, keepdims=False)
    sent = lax.dynamic_index_in_dim(part, 1 - z, 1, keepdims=False)
    part = kept + lax.ppermute(sent, "row_1", [(0, 1), (1, 0)])
    x = lax.axis_index("row_0")
    total = lax.dynamic_index_in_dim(part, x, 0, keepdims=False)
    for k in range(1, 4):
        sent = lax.dynamic_index_in_dim(part, (x + k) % 4, 0, keepdims=False)
        total = total + lax.ppermute(sent, "row_0", [(s, (s + k) % 4) for s in range(4)])
    return total


def solution(mesh):
    split = Mesh(mesh.devices.reshape(4, 2, 2, 4, 2), ROW_COL)
    return jax.shard_map(
        per_device,
        mesh=split,
        in_specs=(P(ROW_COL, None), P(None, ROW), P(ROW, COL), P(ROW, COL), P(), P()),
        out_specs=P(ROW, COL),
        check_vma=False,
    )
```

```python
import jax
import jax.numpy as jnp
from jax import lax
from jax.experimental import pallas as pl
from jax.experimental.pallas import tpu as pltpu
from jax.sharding import Mesh
from jax.sharding import PartitionSpec as P

BLK = 128
ROW = ("row_0", "row_1", "row_2")
COL = ("col_0", "col_1")
ROW_COL = ROW + COL
CHIPS = ("row_0", "row_1", "col_0", "col_1")
F32 = jnp.float32
BF16 = jnp.bfloat16
SENT = 5


def dot_bf16(a, b):
    return jnp.dot(a, b, preferred_element_type=F32)


def halves(x):
    high = x.astype(BF16)
    return high, (x - high.astype(F32)).astype(BF16)


def dot_three(a, b_high, b_low):
    high, low = halves(a)
    return dot_bf16(high, b_high) + (dot_bf16(high, b_low) + dot_bf16(low, b_high))


def lane_copy(x, column):
    return jnp.take_along_axis(x, jnp.full((8, BLK), column, jnp.int32), axis=1)


def row_copy(x, row):
    return jnp.broadcast_to(x[row : row + 1, :], (8, BLK))


def factor_panels(rows, sub, lane):
    groups = len(rows)
    late = []

    def flush(chosen):
        for g, update in [item for item in late if item[0] in chosen]:
            update()
        late[:] = [item for item in late if item[0] not in chosen]

    for t in range(0, groups, 2):
        first = 8 * t
        flush((t, t + 1))
        pivot = [[], []]
        for m in range(16):
            for y in range(2):
                pivot[y].append(lane_copy(rows[t + y], first + m))
        below = {g: [] for g in range(t + 2, groups)}
        near = [g for g in below if g < t + 4]
        flush(near)
        for m in range(16):
            for g in near:
                below[g].append(lane_copy(rows[g], first + m))
        flush(range(groups))
        for m in range(16):
            for g in range(t + 4, groups):
                below[g].append(lane_copy(rows[g], first + m))
        here = (lane >= first) & (lane < first + 16)
        full = [
            jnp.where(here, jnp.where(lane - first - 8 * y == sub, 1.0, 0.0), rows[t + y])
            for y in range(2)
        ]
        result = list(full)
        inverses = []
        for k in range(0, 16, 2):
            x, i = k // 8, k % 8
            a = row_copy(pivot[x][k], i)
            b = row_copy(pivot[x][k + 1], i)
            c = row_copy(pivot[x][k + 1], i + 1)
            det = a * c - b * b
            root = lax.rsqrt(det)
            q = root * root
            left = []
            for y in range(2):
                u, v = pivot[y][k], pivot[y][k + 1]
                u, v = u * c - v * b, v * a - u * b
                if y == x:
                    others = (sub < i) | (sub > i + 1)
                    u, v = jnp.where(others, u, 0.0), jnp.where(others, v, 0.0)
                left.append((u, v))
            for m in range(k + 2, 16):
                top, low = row_copy(pivot[x][m], i), row_copy(pivot[x][m], i + 1)
                for y in range(2):
                    pivot[y][m] = pivot[y][m] - (left[y][0] * top + left[y][1] * low) * q
            top, low = row_copy(full[x], i), row_copy(full[x], i + 1)
            for y in range(2):
                full[y] = full[y] - (left[y][0] * top + left[y][1] * low) * q
            root_a = lax.rsqrt(a)
            over_a = root_a * root_a
            root_c = lax.rsqrt(det * over_a)
            result[x] = jnp.where(
                sub == i,
                top * root_a,
                jnp.where(sub == i + 1, (low - b * over_a * top) * root_c, result[x]),
            )
            inverses.append((q * a, q * b, q * c))
        rows[t], rows[t + 1] = result
        if below:
            lines = []
            for k in range(0, 16, 2):
                qa, qb, qc = inverses[k // 2]
                top = row_copy(full[k // 8], k % 8)
                low = row_copy(full[k // 8], k % 8 + 1)
                lines += [qc * top - qb * low, qa * low - qb * top]

            def update(g, lines=lines, below=below, here=here):
                terms = [a * b for a, b in zip(below[g], lines)]
                while len(terms) > 1:
                    terms = [a + b for a, b in zip(terms[::2], terms[1::2])]
                rows[g] = jnp.where(here, 0.0, rows[g]) - terms[0]

            for g in below:
                if g in near:
                    update(g)
                else:
                    late.append((g, lambda g=g, update=update: update(g)))
        yield


def kernel(
    where_ref, inv_mask, ks_mask, mine_ref, other_ref, coupling_hbm, lead_hbm, tail_hbm,
    kept_ref, sent_ref,
    m_ref, coupling_ref, lead_ref, tail_ref, ch_ref, cl_ref, kh_ref, kl_ref, th_ref, tl_ref,
    before_ref, right_even, right_odd, left_ref, sem, strip_sem,
):
    right_refs = (right_even, right_odd)
    size = m_ref.shape[0]
    count = size // BLK
    row, col, core = where_ref[0], where_ref[1], where_ref[2]
    copies = [
        pltpu.make_async_copy(coupling_hbm, coupling_ref, sem.at[0]),
        pltpu.make_async_copy(lead_hbm, lead_ref, sem.at[1]),
        pltpu.make_async_copy(tail_hbm, tail_ref, sem.at[2]),
    ]
    sub = lax.broadcasted_iota(jnp.int32, (8, BLK), 0)
    lane = lax.broadcasted_iota(jnp.int32, (8, BLK), 1)

    def at(i):
        return slice(i * BLK, (i + 1) * BLK)

    strips = {b: [] for b in range(count)}
    folds = {b: [] for b in range(count)}
    sems = iter(range(strip_sem.shape[0]))
    for b in range(count):
        for ref, part in ((mine_ref, core), (other_ref, 1 - core)):
            held = pl.ds(pl.multiple_of(b * BLK + part * 64, 64), 64)
            direct = min(SENT, count - b) * BLK
            strips[b].append(
                pltpu.make_async_copy(
                    ref.at[b, :, pl.ds(0, direct)],
                    m_ref.at[held, pl.ds(b * BLK, direct)],
                    strip_sem.at[next(sems)],
                )
            )
            for o in range(count - b, SENT - 1):
                c = b + o - count
                strips[b].append(
                    pltpu.make_async_copy(
                        ref.at[b, :, pl.ds(o * BLK, BLK)],
                        m_ref.at[held, pl.ds(c * BLK, BLK)],
                        strip_sem.at[next(sems)],
                    )
                )
    for b in range(count):
        for copy in strips[b]:
            copy.start()
    for copy in copies:
        copy.start()
    for copy in strips[0]:
        copy.wait()

    def arrive():
        for b in range(1, count):
            for copy in strips[b]:
                copy.wait()
        yield
        for b in range(SENT, count):
            for c in range(b - SENT + 1):
                m_ref[at(c), at(b)] = m_ref[at(b), at(c)].T
            yield

    def prepare():
        for copy in copies:
            copy.wait()
        for k in range(count):
            ch_ref[at(k), :], cl_ref[at(k), :] = halves(coupling_ref[at(k), :])
            yield
        for k in range(count):
            for n in range(lead_ref.shape[1] // BLK):
                keep = ks_mask[row * count + k, col * 4 + n].astype(F32)
                kh_ref[at(k), at(n)], kl_ref[at(k), at(n)] = halves(lead_ref[at(k), at(n)] * keep)
            yield
        th_ref[...] = jnp.zeros(th_ref.shape, BF16)
        tl_ref[...] = jnp.zeros(tl_ref.shape, BF16)
        lead_blocks = ks_mask.shape[0] - count
        for n in range(lead_ref.shape[1] // BLK):
            keep = ks_mask[lead_blocks + row // 2, col * 4 + n].astype(F32)
            high, low = halves(tail_ref[:, at(n)] * keep)
            th_ref[pl.ds(core * 64, 64), at(n)] = high
            tl_ref[pl.ds(core * 64, 64), at(n)] = low
        yield

    def stack(ref, cols, value):
        high, low = halves(value)
        ref[0:BLK, cols] = high
        ref[BLK : 2 * BLK, cols] = high
        ref[2 * BLK :, cols] = low

    def beside(value):
        high, low = halves(value)
        return jnp.concatenate([high, low, high], axis=1)

    def eliminate(j, i, parts):
        right = right_refs[j % 2]
        left = left_ref[i]
        for cols in parts:
            start, stop = cols.start, cols.stop
            update = dot_bf16(left, right[:, cols])
            if start == j * BLK and stop == start + BLK:
                m_ref[at(i), cols] = -update
            else:
                m_ref[at(i), cols] -= update

    def prepare_row(j):
        if j > 0:
            stack(before_ref, slice(0, j * BLK), m_ref[at(j), : j * BLK])
            yield
        if j + 1 < count:
            stack(before_ref, slice((j + 1) * BLK, size), m_ref[at(j), (j + 1) * BLK :])
            yield

    def trailing(j, i, first):
        if not first:
            left_ref[i] = beside(m_ref[at(j), at(i)].T)
        parts = [slice(c * BLK, (c + 1) * BLK) for c in (j,)]
        if j > 0:
            parts.append(slice(0, j * BLK))
        start = (i + 1 if first else i) * BLK
        if start < size:
            parts.append(slice(start, size))
        for part in parts:
            eliminate(j, i, [part])
            yield

    def project(i):
        depth = slice(0, (i + 1) * BLK)
        right = right_refs[i % 2]
        high, low = right[0:BLK, depth], right[2 * BLK :, depth]
        total = None
        for k in range(0, count, 2):
            wide = slice(k * BLK, (k + 2) * BLK)
            lead = dot_bf16(high, ch_ref[depth, wide]) + (
                dot_bf16(high, cl_ref[depth, wide]) + dot_bf16(low, ch_ref[depth, wide])
            )
            keep = [inv_mask[i, row * count + k + q].astype(F32) for q in range(2)]
            lead = jnp.concatenate([lead[:, :BLK] * keep[0], lead[:, BLK:] * keep[1]], axis=1)
            part = dot_three(lead, kh_ref[wide, :], kl_ref[wide, :])
            total = part if total is None else total + part
            yield
        mine = m_ref[at(i), pl.ds(pl.multiple_of(row // 2 * BLK, BLK), BLK)]
        keep = inv_mask[i, inv_mask.shape[1] - count + row // 2]
        mine = jnp.where((keep != 0) & (row // 2 <= i), mine, 0.0)
        total = dot_three(mine, th_ref[...], tl_ref[...]) - total
        half = BLK // 2
        kept_ref[i] = jnp.where(core == 0, total[:half], total[half:])
        sent_ref[i] = jnp.where(core == 0, total[half:], total[:half])
        yield

    fillers = [arrive(), prepare_row(0), prepare()]
    for j in range(count):
        rows = [m_ref[j * BLK + 8 * g : j * BLK + 8 * g + 8, at(j)] for g in range(16)]
        for step in factor_panels(rows, sub, lane):
            for _ in range(5):
                while fillers:
                    try:
                        next(fillers[0])
                        break
                    except StopIteration:
                        fillers.pop(0)
        while fillers:
            for _ in fillers.pop(0):
                pass
        p = jnp.concatenate([jnp.where(lane <= sub + 8 * g, rows[g], 0.0) for g in range(16)], axis=0)
        right = right_refs[j % 2]
        left = beside(p)
        m_ref[at(j), at(j)] = p
        stack(right, at(j), p)
        if j + 1 < count:
            u = dot_bf16(left, before_ref[:, at(j + 1)])
            m_ref[at(j), at(j + 1)] = u
            stack(right, at(j + 1), u)
            left_ref[j + 1] = beside(u.T)
            eliminate(j, j + 1, [at(j + 1)])
        spans = [slice(0, j * BLK)] if j > 0 else []
        if j + 2 < count:
            spans.append(slice((j + 2) * BLK, size))
        for span in spans:
            u = dot_bf16(left, before_ref[:, span])
            m_ref[at(j), span] = u
            stack(right, span, u)
        fillers = []
        if j + 1 < count:
            fillers += [trailing(j, j + 1, True), prepare_row(j + 1)]
        fillers += [trailing(j, i, False) for i in range(j + 2, count)] + [project(j)]
    while fillers:
        for _ in fillers.pop(0):
            pass


def projected_part(place, inv_mask, ks_mask, mine, other, coupling, ks_lead, ks_tail):
    size = coupling.shape[0]
    lead, width = ks_lead.shape
    vmem = pl.BlockSpec(memory_space=pltpu.VMEM)
    smem = pl.BlockSpec(memory_space=pltpu.SMEM)
    hbm = pl.BlockSpec(memory_space=pl.ANY)
    return pl.pallas_call(
        kernel,
        out_shape=[jax.ShapeDtypeStruct((size // BLK, BLK // 2, width), F32)] * 2,
        in_specs=[smem, smem, smem, hbm, hbm, hbm, hbm, hbm],
        out_specs=[vmem, vmem],
        scratch_shapes=[
            pltpu.VMEM((size, size), F32),
            pltpu.VMEM(coupling.shape, F32),
            pltpu.VMEM(ks_lead.shape, F32),
            pltpu.VMEM(ks_tail.shape, F32),
            pltpu.VMEM(coupling.shape, BF16),
            pltpu.VMEM(coupling.shape, BF16),
            pltpu.VMEM(ks_lead.shape, BF16),
            pltpu.VMEM(ks_lead.shape, BF16),
            pltpu.VMEM((BLK, width), BF16),
            pltpu.VMEM((BLK, width), BF16),
            pltpu.VMEM((3 * BLK, size), BF16),
            pltpu.VMEM((3 * BLK, size), BF16),
            pltpu.VMEM((3 * BLK, size), BF16),
            pltpu.VMEM((size // BLK, BLK, 3 * BLK), BF16),
            pltpu.SemaphoreType.DMA((3,)),
            pltpu.SemaphoreType.DMA((28,)),
        ],
        compiler_params=pltpu.CompilerParams(vmem_limit_bytes=48 * 1024 * 1024),
        name="project",
    )(place, inv_mask, ks_mask, mine, other, coupling, ks_lead, ks_tail)


def pieces_first(where_ref, kept, got, z_kept, z_sent, x_own, *x_sent):
    x, z = where_ref[0], where_ref[1]
    half = kept.shape[-1] // 2
    lo, hi = slice(0, half), slice(half, 2 * half)
    for i in range(4):
        z_kept[i] = kept[2 * i + z, :, lo] + got[2 * i + z, :, lo]
        z_sent[i] = kept[2 * i + 1 - z, :, lo] + got[2 * i + 1 - z, :, lo]
    for k, ref in enumerate((x_own, *x_sent)):
        to = lax.rem(x + k, 4)
        for i in range(2):
            ref[i] = kept[2 * to + i, :, hi] + got[2 * to + i, :, hi]


def pieces_second(where_ref, z_kept, z_got, x_own, x1, x2, x3, y_own, y1, y2, y3, v_kept, v_sent):
    x, z = where_ref[0], where_ref[1]
    for k, ref in enumerate((y_own, y1, y2, y3)):
        to = lax.rem(x + k, 4)
        ref[...] = z_kept[to] + z_got[to]
    for ref, i in ((v_kept, z), (v_sent, 1 - z)):
        ref[...] = (x_own[i] + x1[i]) + (x2[i] + x3[i])


def pieces_third(y_own, y1, y2, y3, v_kept, v_got, out):
    half = out.shape[-1] // 2
    out[:, :half] = (y_own[...] + y1[...]) + (y2[...] + y3[...])
    out[:, half:] = v_kept[...] + v_got[...]


def summed(where, kept, sent):
    vmem = pl.BlockSpec(memory_space=pltpu.VMEM)
    smem = pl.BlockSpec(memory_space=pltpu.SMEM)
    swap = [(0, 1), (1, 0)]
    rows, half = kept.shape[1], kept.shape[2] // 2

    def shape(*lead):
        return jax.ShapeDtypeStruct((*lead, rows, half), F32)

    def turned(parts):
        return [
            lax.ppermute(part, "row_0", [(s, (s + k) % 4) for s in range(4)])
            for k, part in zip((1, 2, 3), parts)
        ]

    got = lax.ppermute(sent, "row_2", swap)
    z_kept, z_sent, x_own, *x_sent = pl.pallas_call(
        pieces_first,
        out_shape=[shape(4), shape(4)] + [shape(2)] * 4,
        in_specs=[smem, vmem, vmem],
        out_specs=[vmem] * 6,
        name="pieces_first",
    )(where, kept, got)
    z_got = lax.ppermute(z_sent, "row_1", swap)
    x_got = turned(x_sent)
    y_own, y1, y2, y3, v_kept, v_sent = pl.pallas_call(
        pieces_second,
        out_shape=[shape()] * 6,
        in_specs=[smem] + [vmem] * 6,
        out_specs=[vmem] * 6,
        name="pieces_second",
    )(where, z_kept, z_got, x_own, *x_got)
    v_got = lax.ppermute(v_sent, "row_1", swap)
    y_got = turned((y1, y2, y3))
    return pl.pallas_call(
        pieces_third,
        out_shape=jax.ShapeDtypeStruct((rows, 2 * half), F32),
        in_specs=[vmem] * 6,
        out_specs=vmem,
        name="pieces_third",
    )(y_own, *y_got, v_kept, v_got)


def per_device(schur_tail, coupling, ks_lead, ks_tail, inv_mask, ks_mask):
    row_index = lax.axis_index(ROW)
    col_index = lax.axis_index(COL)
    core_index = lax.axis_index("row_2")
    twice = jnp.concatenate([schur_tail, schur_tail[:, : SENT * BLK - BLK]], axis=1)
    strip = lax.dynamic_slice_in_dim(twice, row_index // 2 * BLK, SENT * BLK, 1)
    chips = 1
    for axis in CHIPS:
        chips *= lax.axis_size(axis)
    copies = jnp.broadcast_to(strip[None], (chips,) + strip.shape)
    mine = lax.all_to_all(copies, CHIPS, split_axis=0, concat_axis=0, tiled=True)
    mine = mine.reshape(-1, BLK // 2, SENT * BLK)
    other = lax.ppermute(mine, "row_2", [(0, 1), (1, 0)])
    place = jnp.stack([row_index, col_index, core_index]).astype(jnp.int32)
    kept, sent = projected_part(place, inv_mask, ks_mask, mine, other, coupling, ks_lead, ks_tail)
    where = jnp.stack([lax.axis_index("row_0"), lax.axis_index("row_1")]).astype(jnp.int32)
    return summed(where, kept, sent)


def solution(mesh):
    split = Mesh(mesh.devices.reshape(4, 2, 2, 4, 2), ROW_COL)
    return jax.shard_map(
        per_device,
        mesh=split,
        in_specs=(P(ROW_COL, None), P(None, ROW), P(ROW, COL), P(ROW, COL), P(), P()),
        out_specs=P(ROW, COL),
        check_vma=False,
    )
```

```python
import jax
import jax.numpy as jnp
from jax import lax
from jax.experimental import pallas as pl
from jax.experimental.pallas import tpu as pltpu
from jax.sharding import Mesh
from jax.sharding import PartitionSpec as P

BLK = 128
ROW = ("row_0", "row_1", "row_2")
COL = ("col_0", "col_1")
ROW_COL = ROW + COL
CHIPS = ("row_0", "row_1", "col_0", "col_1")
F32 = jnp.float32
BF16 = jnp.bfloat16
SENT = 5


def dot_bf16(a, b):
    return jnp.dot(a, b, preferred_element_type=F32)


def halves(x):
    high = x.astype(BF16)
    return high, (x - high.astype(F32)).astype(BF16)


def dot_three(a, b_high, b_low):
    high, low = halves(a)
    return dot_bf16(high, b_high) + (dot_bf16(high, b_low) + dot_bf16(low, b_high))


def lane_copy(x, column):
    return jnp.take_along_axis(x, jnp.full((8, BLK), column, jnp.int32), axis=1)


def row_copy(x, row):
    return jnp.broadcast_to(x[row : row + 1, :], (8, BLK))


def factor_panels(rows, sub, lane, lines_ref):
    groups = len(rows)
    for t in range(0, groups, 2):
        first = 8 * t
        pivot = [[], []]
        for m in range(16):
            for y in range(2):
                pivot[y].append(lane_copy(rows[t + y], first + m))
        near = range(t + 2, min(groups, t + 6))
        far = range(t + 6, groups)
        below = {g: [] for g in near}
        for pair in range(0, len(near), 2):
            for m in range(16):
                for g in near[pair : pair + 2]:
                    below[g].append(lane_copy(rows[g], first + m))
        here = (lane >= first) & (lane < first + 16)
        full = [
            jnp.where(here, jnp.where(lane - first - 8 * y == sub, 1.0, 0.0), rows[t + y])
            for y in range(2)
        ]
        result = list(full)
        inverses = []
        for k in range(0, 16, 2):
            x, i = k // 8, k % 8
            a = row_copy(pivot[x][k], i)
            b = row_copy(pivot[x][k + 1], i)
            c = row_copy(pivot[x][k + 1], i + 1)
            det = a * c - b * b
            root = lax.rsqrt(det)
            q = root * root
            left = []
            for y in range(2):
                u, v = pivot[y][k], pivot[y][k + 1]
                u, v = u * c - v * b, v * a - u * b
                if y == x:
                    others = (sub < i) | (sub > i + 1)
                    u, v = jnp.where(others, u, 0.0), jnp.where(others, v, 0.0)
                left.append((u, v))
            for m in range(k + 2, 16):
                top, low = row_copy(pivot[x][m], i), row_copy(pivot[x][m], i + 1)
                for y in range(2):
                    pivot[y][m] = pivot[y][m] - (left[y][0] * top + left[y][1] * low) * q
            top, low = row_copy(full[x], i), row_copy(full[x], i + 1)
            for y in range(2):
                full[y] = full[y] - (left[y][0] * top + left[y][1] * low) * q
            root_a = lax.rsqrt(a)
            over_a = root_a * root_a
            root_c = lax.rsqrt(det * over_a)
            result[x] = jnp.where(
                sub == i,
                top * root_a,
                jnp.where(sub == i + 1, (low - b * over_a * top) * root_c, result[x]),
            )
            inverses.append((q * a, q * b, q * c))
        rows[t], rows[t + 1] = result
        if below:
            lines = []
            for k in range(0, 16, 2):
                qa, qb, qc = inverses[k // 2]
                top = row_copy(full[k // 8], k % 8)
                low = row_copy(full[k // 8], k % 8 + 1)
                lines += [qc * top - qb * low, qa * low - qb * top]

            for g in near:
                terms = [a * b for a, b in zip(below[g], lines)]
                while len(terms) > 1:
                    terms = [a + b for a, b in zip(terms[::2], terms[1::2])]
                rows[g] = jnp.where(here, 0.0, rows[g]) - terms[0]
        if far:
            tall = []
            for y in range(2):
                value = lines[8 * y]
                for i in range(1, 8):
                    value = jnp.where(sub == i, lines[8 * y + i], value)
                tall.append(value)
            high, low = halves(jnp.concatenate(tall, axis=0))
            for part, value in enumerate((high, high, low)):
                lines_ref[t // 2, part * BLK + first : part * BLK + first + 16, :] = value
            high, low = halves(jnp.concatenate([rows[g] for g in far], axis=0))
            update = dot_bf16(jnp.concatenate([high, low, high], axis=1), lines_ref[t // 2])
            for i, g in enumerate(far):
                rows[g] = jnp.where(here, 0.0, rows[g]) - update[8 * i : 8 * i + 8]
        yield


def at_ds(i):
    return pl.ds(i * BLK, BLK)


def kernel(
    where_ref, inv_mask, ks_mask, mine_ref, other_ref, coupling_hbm, lead_hbm, tail_hbm,
    kept_ref, sent_ref,
    m_ref, coupling_ref, lead_ref, tail_ref, ch_ref, cl_ref, kh_ref, kl_ref, th_ref, tl_ref,
    before_ref, right_even, right_odd, left_ref, lines_ref, last_ref, sem, strip_sem,
):
    right_refs = (right_even, right_odd)
    size = m_ref.shape[0]
    count = size // BLK
    row, col, core = where_ref[0], where_ref[1], where_ref[2]
    lead_copies = [
        pltpu.make_async_copy(lead_hbm.at[at_ds(k), :], lead_ref.at[at_ds(k), :], sem.at[k])
        for k in range(count)
    ]
    coupling_copies = [
        pltpu.make_async_copy(
            coupling_hbm.at[at_ds(k), :], coupling_ref.at[at_ds(k), :], sem.at[count + k]
        )
        for k in range(count)
    ]
    tail_copy = pltpu.make_async_copy(tail_hbm, tail_ref, sem.at[2 * count])
    sub = lax.broadcasted_iota(jnp.int32, (8, BLK), 0)
    lane = lax.broadcasted_iota(jnp.int32, (8, BLK), 1)

    def at(i):
        return slice(i * BLK, (i + 1) * BLK)

    strips = {b: [] for b in range(count)}
    folds = {b: [] for b in range(count)}
    sems = iter(range(strip_sem.shape[0]))
    for b in range(count):
        for ref, part in ((mine_ref, core), (other_ref, 1 - core)):
            held = pl.ds(pl.multiple_of(b * BLK + part * 64, 64), 64)
            direct = min(SENT, count - b) * BLK
            strips[b].append(
                pltpu.make_async_copy(
                    ref.at[b, :, pl.ds(0, direct)],
                    m_ref.at[held, pl.ds(b * BLK, direct)],
                    strip_sem.at[next(sems)],
                )
            )
            for o in range(count - b, SENT - 1):
                c = b + o - count
                strips[b].append(
                    pltpu.make_async_copy(
                        ref.at[b, :, pl.ds(o * BLK, BLK)],
                        m_ref.at[held, pl.ds(c * BLK, BLK)],
                        strip_sem.at[next(sems)],
                    )
                )
    for b in range(count):
        for copy in strips[b]:
            copy.start()
    tail_copy.start()
    for k in range(count):
        lead_copies[k].start()
    for k in range(count):
        coupling_copies[k].start()
    lines_ref[...] = jnp.zeros(lines_ref.shape, BF16)
    for copy in strips[0]:
        copy.wait()

    def arrive():
        for b in range(1, count):
            for copy in strips[b]:
                copy.wait()
        yield
        for b in range(SENT, count):
            for c in range(b - SENT + 1):
                m_ref[at(c), at(b)] = m_ref[at(b), at(c)].T
            yield

    def pause(steps):
        for _ in range(steps):
            yield

    def split_coupling(k):
        coupling_copies[k].wait()
        for half in range(2):
            wide = slice(half * size // 2, (half + 1) * size // 2)
            ch_ref[at(k), wide], cl_ref[at(k), wide] = halves(coupling_ref[at(k), wide])
            yield

    def prepare():
        for k in range(count):
            lead_copies[k].wait()
            for n in range(lead_ref.shape[1] // BLK):
                keep = ks_mask[row * count + k, col * 4 + n].astype(F32)
                kh_ref[at(k), at(n)], kl_ref[at(k), at(n)] = halves(lead_ref[at(k), at(n)] * keep)
            yield
        tail_copy.wait()
        th_ref[...] = jnp.zeros(th_ref.shape, BF16)
        tl_ref[...] = jnp.zeros(tl_ref.shape, BF16)
        lead_blocks = ks_mask.shape[0] - count
        for n in range(lead_ref.shape[1] // BLK):
            keep = ks_mask[lead_blocks + row // 2, col * 4 + n].astype(F32)
            high, low = halves(tail_ref[:, at(n)] * keep)
            th_ref[pl.ds(core * 64, 64), at(n)] = high
            tl_ref[pl.ds(core * 64, 64), at(n)] = low
        yield

    def stack(ref, cols, value):
        high, low = halves(value)
        ref[0:BLK, cols] = high
        ref[BLK : 2 * BLK, cols] = high
        ref[2 * BLK :, cols] = low

    def beside(value):
        high, low = halves(value)
        return jnp.concatenate([high, low, high], axis=1)

    def eliminate(j, i, parts):
        right = right_refs[j % 2]
        left = left_ref[i]
        for cols in parts:
            start, stop = cols.start, cols.stop
            update = dot_bf16(left, right[:, cols])
            if start == j * BLK and stop == start + BLK:
                m_ref[at(i), cols] = -update
            else:
                m_ref[at(i), cols] -= update

    def prepare_row(j):
        if j > 0:
            stack(before_ref, slice(0, j * BLK), m_ref[at(j), : j * BLK])
            yield
        if j + 1 < count:
            stack(before_ref, slice((j + 1) * BLK, size), m_ref[at(j), (j + 1) * BLK :])
            yield

    def trailing(j, i, first):
        if not first:
            left_ref[i] = beside(m_ref[at(j), at(i)].T)
        parts = [slice(c * BLK, (c + 1) * BLK) for c in (j,)]
        if j > 0:
            parts.append(slice(0, j * BLK))
        start = (i + 1 if first else i) * BLK
        if start < size:
            parts.append(slice(start, size))
        for part in parts:
            eliminate(j, i, [part])
            yield

    def early_lead():
        coupling_copies[count - 1].wait()
        depth = slice(0, size - BLK)
        high, low = before_ref[0:BLK, depth], before_ref[2 * BLK :, depth]
        for k in range(0, count, 2):
            wide = slice(k * BLK, (k + 2) * BLK)
            value = coupling_ref[size - BLK :, wide] + (
                dot_bf16(high, ch_ref[depth, wide])
                + (dot_bf16(high, cl_ref[depth, wide]) + dot_bf16(low, ch_ref[depth, wide]))
            )
            stack(last_ref, wide, value)
            yield

    def project(i, left):
        depth = slice(0, (i + 1) * BLK)
        right = right_refs[i % 2]
        high, low = right[0:BLK, depth], right[2 * BLK :, depth]
        total = None
        for k in range(0, count, 2):
            wide = slice(k * BLK, (k + 2) * BLK)
            if i + 1 == count:
                lead = dot_bf16(left, last_ref[:, wide])
            else:
                lead = dot_bf16(high, ch_ref[depth, wide]) + (
                    dot_bf16(high, cl_ref[depth, wide]) + dot_bf16(low, ch_ref[depth, wide])
                )
            keep = [inv_mask[i, row * count + k + q].astype(F32) for q in range(2)]
            lead = jnp.concatenate([lead[:, :BLK] * keep[0], lead[:, BLK:] * keep[1]], axis=1)
            part = dot_three(lead, kh_ref[wide, :], kl_ref[wide, :])
            total = part if total is None else total + part
            yield
        mine = m_ref[at(i), pl.ds(pl.multiple_of(row // 2 * BLK, BLK), BLK)]
        keep = inv_mask[i, inv_mask.shape[1] - count + row // 2]
        mine = jnp.where((keep != 0) & (row // 2 <= i), mine, 0.0)
        total = dot_three(mine, th_ref[...], tl_ref[...]) - total
        half = BLK // 2
        kept_ref[i] = jnp.where(core == 0, total[:half], total[half:])
        sent_ref[i] = jnp.where(core == 0, total[half:], total[:half])
        yield

    fillers = [arrive(), prepare_row(0), pause(6), prepare(), split_coupling(0)]
    for j in range(count):
        rows = [m_ref[j * BLK + 8 * g : j * BLK + 8 * g + 8, at(j)] for g in range(16)]
        for step in factor_panels(rows, sub, lane, lines_ref):
            for _ in range(4):
                while fillers:
                    try:
                        next(fillers[0])
                        break
                    except StopIteration:
                        fillers.pop(0)
        while fillers:
            for _ in fillers.pop(0):
                pass
        p = jnp.concatenate([jnp.where(lane <= sub + 8 * g, rows[g], 0.0) for g in range(16)], axis=0)
        right = right_refs[j % 2]
        left = beside(p)
        m_ref[at(j), at(j)] = p
        stack(right, at(j), p)
        if j + 1 < count:
            u = dot_bf16(left, before_ref[:, at(j + 1)])
            m_ref[at(j), at(j + 1)] = u
            stack(right, at(j + 1), u)
            left_ref[j + 1] = beside(u.T)
            eliminate(j, j + 1, [at(j + 1)])
        spans = [slice(0, j * BLK)] if j > 0 else []
        if j + 2 < count:
            spans.append(slice((j + 2) * BLK, size))
        for span in spans:
            u = dot_bf16(left, before_ref[:, span])
            m_ref[at(j), span] = u
            stack(right, span, u)
        fillers = []
        if j + 1 < count:
            fillers += [trailing(j, j + 1, True), prepare_row(j + 1)]
            if j + 2 < count:
                fillers.append(split_coupling(j + 1))
            else:
                fillers.append(early_lead())
        fillers += [trailing(j, i, False) for i in range(j + 2, count)] + [project(j, left)]
    while fillers:
        for _ in fillers.pop(0):
            pass


def projected_part(place, inv_mask, ks_mask, mine, other, coupling, ks_lead, ks_tail):
    size = coupling.shape[0]
    lead, width = ks_lead.shape
    vmem = pl.BlockSpec(memory_space=pltpu.VMEM)
    smem = pl.BlockSpec(memory_space=pltpu.SMEM)
    hbm = pl.BlockSpec(memory_space=pl.ANY)
    return pl.pallas_call(
        kernel,
        out_shape=[jax.ShapeDtypeStruct((size // BLK, BLK // 2, width), F32)] * 2,
        in_specs=[smem, smem, smem, hbm, hbm, hbm, hbm, hbm],
        out_specs=[vmem, vmem],
        scratch_shapes=[
            pltpu.VMEM((size, size), F32),
            pltpu.VMEM(coupling.shape, F32),
            pltpu.VMEM(ks_lead.shape, F32),
            pltpu.VMEM(ks_tail.shape, F32),
            pltpu.VMEM(coupling.shape, BF16),
            pltpu.VMEM(coupling.shape, BF16),
            pltpu.VMEM(ks_lead.shape, BF16),
            pltpu.VMEM(ks_lead.shape, BF16),
            pltpu.VMEM((BLK, width), BF16),
            pltpu.VMEM((BLK, width), BF16),
            pltpu.VMEM((3 * BLK, size), BF16),
            pltpu.VMEM((3 * BLK, size), BF16),
            pltpu.VMEM((3 * BLK, size), BF16),
            pltpu.VMEM((size // BLK, BLK, 3 * BLK), BF16),
            pltpu.VMEM((5, 3 * BLK, BLK), BF16),
            pltpu.VMEM((3 * BLK, size), BF16),
            pltpu.SemaphoreType.DMA((17,)),
            pltpu.SemaphoreType.DMA((28,)),
        ],
        compiler_params=pltpu.CompilerParams(vmem_limit_bytes=36 * 1024 * 1024),
        name="project",
    )(place, inv_mask, ks_mask, mine, other, coupling, ks_lead, ks_tail)


def pieces_first(where_ref, kept, got, z_kept, z_sent, x_own, *x_sent):
    x, z = where_ref[3], where_ref[4]
    half = kept.shape[-1] // 2
    lo, hi = slice(0, half), slice(half, 2 * half)
    for i in range(4):
        z_kept[i] = kept[2 * i + z, :, lo] + got[2 * i + z, :, lo]
        z_sent[i] = kept[2 * i + 1 - z, :, lo] + got[2 * i + 1 - z, :, lo]
    for k, ref in enumerate((x_own, *x_sent)):
        to = lax.rem(x + k, 4)
        for i in range(2):
            ref[i] = kept[2 * to + i, :, hi] + got[2 * to + i, :, hi]


def pieces_second(where_ref, z_kept, z_got, x_own, x1, x2, x3, y_own, y1, y2, y3, v_kept, v_sent):
    x, z = where_ref[3], where_ref[4]
    for k, ref in enumerate((y_own, y1, y2, y3)):
        to = lax.rem(x + k, 4)
        ref[...] = z_kept[to] + z_got[to]
    for ref, i in ((v_kept, z), (v_sent, 1 - z)):
        ref[...] = (x_own[i] + x1[i]) + (x2[i] + x3[i])


def pieces_third(y_own, y1, y2, y3, v_kept, v_got, out):
    half = out.shape[-1] // 2
    out[:, :half] = (y_own[...] + y1[...]) + (y2[...] + y3[...])
    out[:, half:] = v_kept[...] + v_got[...]


def summed(where, kept, sent):
    vmem = pl.BlockSpec(memory_space=pltpu.VMEM)
    smem = pl.BlockSpec(memory_space=pltpu.SMEM)
    swap = [(0, 1), (1, 0)]
    rows, half = kept.shape[1], kept.shape[2] // 2

    def shape(*lead):
        return jax.ShapeDtypeStruct((*lead, rows, half), F32)

    def turned(parts):
        return [
            lax.ppermute(part, "row_0", [(s, (s + k) % 4) for s in range(4)])
            for k, part in zip((1, 2, 3), parts)
        ]

    got = lax.ppermute(sent, "row_2", swap)
    z_kept, z_sent, x_own, *x_sent = pl.pallas_call(
        pieces_first,
        out_shape=[shape(4), shape(4)] + [shape(2)] * 4,
        in_specs=[smem, vmem, vmem],
        out_specs=[vmem] * 6,
        compiler_params=pltpu.CompilerParams(vmem_limit_bytes=4 * 1024 * 1024),
        name="pieces_first",
    )(where, kept, got)
    z_got = lax.ppermute(z_sent, "row_1", swap)
    x_got = turned(x_sent)
    y_own, y1, y2, y3, v_kept, v_sent = pl.pallas_call(
        pieces_second,
        out_shape=[shape()] * 6,
        in_specs=[smem] + [vmem] * 6,
        out_specs=[vmem] * 6,
        compiler_params=pltpu.CompilerParams(vmem_limit_bytes=4 * 1024 * 1024),
        name="pieces_second",
    )(where, z_kept, z_got, x_own, *x_got)
    v_got = lax.ppermute(v_sent, "row_1", swap)
    y_got = turned((y1, y2, y3))
    return pl.pallas_call(
        pieces_third,
        out_shape=jax.ShapeDtypeStruct((rows, 2 * half), F32),
        in_specs=[vmem] * 6,
        out_specs=vmem,
        compiler_params=pltpu.CompilerParams(vmem_limit_bytes=4 * 1024 * 1024),
        name="pieces_third",
    )(y_own, *y_got, v_kept, v_got)


def per_device(schur_tail, coupling, ks_lead, ks_tail, inv_mask, ks_mask):
    row_index = lax.axis_index(ROW)
    col_index = lax.axis_index(COL)
    core_index = lax.axis_index("row_2")
    twice = jnp.concatenate([schur_tail, schur_tail[:, : SENT * BLK - BLK]], axis=1)
    strip = lax.dynamic_slice_in_dim(twice, row_index // 2 * BLK, SENT * BLK, 1)
    chips = 1
    for axis in CHIPS:
        chips *= lax.axis_size(axis)
    copies = jnp.broadcast_to(strip[None], (chips,) + strip.shape)
    mine = lax.all_to_all(copies, CHIPS, split_axis=0, concat_axis=0, tiled=True)
    mine = mine.reshape(-1, BLK // 2, SENT * BLK)
    other = lax.ppermute(mine, "row_2", [(0, 1), (1, 0)])
    place = jnp.stack(
        [row_index, col_index, core_index, lax.axis_index("row_0"), lax.axis_index("row_1")]
    ).astype(jnp.int32)
    kept, sent = projected_part(place, inv_mask, ks_mask, mine, other, coupling, ks_lead, ks_tail)
    return summed(place, kept, sent)


def solution(mesh):
    split = Mesh(mesh.devices.reshape(4, 2, 2, 4, 2), ROW_COL)
    return jax.shard_map(
        per_device,
        mesh=split,
        in_specs=(P(ROW_COL, None), P(None, ROW), P(ROW, COL), P(ROW, COL), P(), P()),
        out_specs=P(ROW, COL),
        check_vma=False,
    )
```

```python
import jax
import jax.numpy as jnp
from jax import lax
from jax.experimental import pallas as pl
from jax.experimental.pallas import tpu as pltpu
from jax.sharding import Mesh
from jax.sharding import PartitionSpec as P

BLK = 128
ROW = ("row_0", "row_1", "row_2")
COL = ("col_0", "col_1")
ROW_COL = ROW + COL
CHIPS = ("row_0", "row_1", "col_0", "col_1")
F32 = jnp.float32
BF16 = jnp.bfloat16
SENT = 5


def dot_bf16(a, b):
    return jnp.dot(a, b, preferred_element_type=F32)


def halves(x):
    high = x.astype(BF16)
    return high, (x - high.astype(F32)).astype(BF16)


def lane_copy(x, column):
    return jnp.take_along_axis(x, jnp.full((8, BLK), column, jnp.int32), axis=1)


def row_copy(x, row):
    return jnp.broadcast_to(x[row : row + 1, :], (8, BLK))


def factor_panels(rows, sub, lane, lines_ref):
    groups = len(rows)
    for t in range(0, groups, 2):
        first = 8 * t
        pivot = [[], []]
        for m in range(16):
            for y in range(2):
                pivot[y].append(lane_copy(rows[t + y], first + m))
        near = range(t + 2, min(groups, t + 6))
        far = range(t + 6, groups)
        below = {g: [] for g in near}
        for pair in range(0, len(near), 2):
            for m in range(16):
                for g in near[pair : pair + 2]:
                    below[g].append(lane_copy(rows[g], first + m))
        here = (lane >= first) & (lane < first + 16)
        full = [
            jnp.where(here, jnp.where(lane - first - 8 * y == sub, 1.0, 0.0), rows[t + y])
            for y in range(2)
        ]
        result = list(full)
        inverses = []
        for k in range(0, 16, 2):
            x, i = k // 8, k % 8
            a = row_copy(pivot[x][k], i)
            b = row_copy(pivot[x][k + 1], i)
            c = row_copy(pivot[x][k + 1], i + 1)
            det = a * c - b * b
            root = lax.rsqrt(det)
            q = root * root
            left = []
            for y in range(2):
                u, v = pivot[y][k], pivot[y][k + 1]
                u, v = u * c - v * b, v * a - u * b
                if y == x:
                    others = (sub < i) | (sub > i + 1)
                    u, v = jnp.where(others, u, 0.0), jnp.where(others, v, 0.0)
                left.append((u, v))
            for m in range(k + 2, min(k + 4, 16)):
                top, low = row_copy(pivot[x][m], i), row_copy(pivot[x][m], i + 1)
                for y in range(2):
                    pivot[y][m] = pivot[y][m] - (left[y][0] * top + left[y][1] * low) * q
            left = [(u * q, v * q) for u, v in left]
            for m in range(k + 4, 16):
                top, low = row_copy(pivot[x][m], i), row_copy(pivot[x][m], i + 1)
                for y in range(2):
                    pivot[y][m] = pivot[y][m] - (left[y][0] * top + left[y][1] * low)
            top, low = row_copy(full[x], i), row_copy(full[x], i + 1)
            for y in range(2):
                full[y] = full[y] - (left[y][0] * top + left[y][1] * low)
            root_a = lax.rsqrt(a)
            over_a = root_a * root_a
            root_c = lax.rsqrt(det * over_a)
            result[x] = jnp.where(
                sub == i,
                top * root_a,
                jnp.where(sub == i + 1, (low - b * over_a * top) * root_c, result[x]),
            )
            inverses.append((q * a, q * b, q * c))
        rows[t], rows[t + 1] = result
        if below:
            lines = []
            for k in range(0, 16, 2):
                qa, qb, qc = inverses[k // 2]
                top = row_copy(full[k // 8], k % 8)
                low = row_copy(full[k // 8], k % 8 + 1)
                lines += [qc * top - qb * low, qa * low - qb * top]

            for g in near:
                terms = [a * b for a, b in zip(below[g], lines)]
                while len(terms) > 1:
                    terms = [a + b for a, b in zip(terms[::2], terms[1::2])]
                rows[g] = jnp.where(here, 0.0, rows[g]) - terms[0]
        if far:
            tall = []
            for y in range(2):
                value = lines[8 * y]
                for i in range(1, 8):
                    value = jnp.where(sub == i, lines[8 * y + i], value)
                tall.append(value)
            high, low = halves(jnp.concatenate(tall, axis=0))
            for part, value in enumerate((high, high, low)):
                lines_ref[t // 2, part * BLK + first : part * BLK + first + 16, :] = value
            high, low = halves(jnp.concatenate([rows[g] for g in far], axis=0))
            update = dot_bf16(jnp.concatenate([high, low, high], axis=1), lines_ref[t // 2])
            for i, g in enumerate(far):
                rows[g] = jnp.where(here, 0.0, rows[g]) - update[8 * i : 8 * i + 8]
        yield


def at_ds(i):
    return pl.ds(i * BLK, BLK)


def kernel(
    where_ref, inv_mask, ks_mask, mine_ref, other_ref, coupling_hbm, lead_hbm, tail_hbm,
    kept_ref, sent_ref,
    m_ref, coupling_ref, lead_ref, tail_ref, c_ref, k_ref, t_ref, x_ref, lead_stack,
    before_ref, right_even, right_odd, left_ref, lines_ref, last_ref, sem, strip_sem,
):
    right_refs = (right_even, right_odd)
    size = m_ref.shape[0]
    count = size // BLK
    row, col, core = where_ref[0], where_ref[1], where_ref[2]
    lead_copies = [
        pltpu.make_async_copy(lead_hbm.at[at_ds(k), :], lead_ref.at[at_ds(k), :], sem.at[k])
        for k in range(count)
    ]
    coupling_copies = [
        pltpu.make_async_copy(
            coupling_hbm.at[at_ds(k), :], coupling_ref.at[at_ds(k), :], sem.at[count + k]
        )
        for k in range(count)
    ]
    tail_copy = pltpu.make_async_copy(tail_hbm, tail_ref, sem.at[2 * count])
    sub = lax.broadcasted_iota(jnp.int32, (8, BLK), 0)
    lane = lax.broadcasted_iota(jnp.int32, (8, BLK), 1)

    def at(i):
        return slice(i * BLK, (i + 1) * BLK)

    strips = {b: [] for b in range(count)}
    folds = {b: [] for b in range(count)}
    sems = iter(range(strip_sem.shape[0]))
    for b in range(count):
        for ref, part in ((mine_ref, core), (other_ref, 1 - core)):
            held = pl.ds(pl.multiple_of(b * BLK + part * 64, 64), 64)
            direct = min(SENT, count - b) * BLK
            strips[b].append(
                pltpu.make_async_copy(
                    ref.at[b, :, pl.ds(0, direct)],
                    m_ref.at[held, pl.ds(b * BLK, direct)],
                    strip_sem.at[next(sems)],
                )
            )
            for o in range(count - b, SENT - 1):
                c = b + o - count
                strips[b].append(
                    pltpu.make_async_copy(
                        ref.at[b, :, pl.ds(o * BLK, BLK)],
                        m_ref.at[held, pl.ds(c * BLK, BLK)],
                        strip_sem.at[next(sems)],
                    )
                )
    for b in range(count):
        for copy in strips[b]:
            copy.start()
    tail_copy.start()
    for k in range(count):
        lead_copies[k].start()
    for k in range(count):
        coupling_copies[k].start()
    lines_ref[...] = jnp.zeros(lines_ref.shape, BF16)
    for copy in strips[0]:
        copy.wait()

    def arrive():
        for b in range(1, count):
            for copy in strips[b]:
                copy.wait()
        yield
        for b in range(SENT, count):
            for c in range(b - SENT + 1):
                m_ref[at(c), at(b)] = m_ref[at(b), at(c)].T
            yield

    def pause(steps):
        for _ in range(steps):
            yield

    def split_coupling(k):
        coupling_copies[k].wait()
        for half in range(2):
            wide = slice(half * size // 2, (half + 1) * size // 2)
            high, low = halves(coupling_ref[at(k), wide])
            for part, value in enumerate((high, high, low)):
                c_ref[at(3 * k + part), wide] = value
            yield

    def prepare():
        for k in range(count):
            lead_copies[k].wait()
            for n in range(lead_ref.shape[1] // BLK):
                keep = ks_mask[row * count + k, col * 4 + n].astype(F32)
                high, low = halves(lead_ref[at(k), at(n)] * keep)
                for part, value in enumerate((high, high, low)):
                    k_ref[at(3 * k + part), at(n)] = value
            yield
        tail_copy.wait()
        t_ref[...] = jnp.zeros(t_ref.shape, BF16)
        lead_blocks = ks_mask.shape[0] - count
        for n in range(lead_ref.shape[1] // BLK):
            keep = ks_mask[lead_blocks + row // 2, col * 4 + n].astype(F32)
            high, low = halves(tail_ref[:, at(n)] * keep)
            for part, value in enumerate((high, high, low)):
                t_ref[pl.ds(pl.multiple_of(part * BLK + core * 64, 64), 64), at(n)] = value
        yield

    def stack(ref, cols, value):
        high, low = halves(value)
        ref[0:BLK, cols] = high
        ref[BLK : 2 * BLK, cols] = high
        ref[2 * BLK :, cols] = low

    def beside(value):
        high, low = halves(value)
        return jnp.concatenate([high, low, high], axis=1)

    def eliminate(j, i, parts):
        right = right_refs[j % 2]
        left = left_ref[i]
        for cols in parts:
            start, stop = cols.start, cols.stop
            update = dot_bf16(left, right[:, cols])
            if start == j * BLK and stop == start + BLK:
                m_ref[at(i), cols] = -update
            else:
                m_ref[at(i), cols] -= update

    def prepare_row(j):
        if j > 0:
            stack(before_ref, slice(0, j * BLK), m_ref[at(j), : j * BLK])
            yield
        if j + 1 < count:
            stack(before_ref, slice((j + 1) * BLK, size), m_ref[at(j), (j + 1) * BLK :])
            yield

    def trailing(j, i, first):
        if not first:
            left_ref[i] = beside(m_ref[at(j), at(i)].T)
        parts = [slice(c * BLK, (c + 1) * BLK) for c in (j,)]
        if j > 0:
            parts.append(slice(0, j * BLK))
        start = (i + 1 if first else i) * BLK
        if start < size:
            parts.append(slice(start, size))
        for part in parts:
            eliminate(j, i, [part])
            yield

    def beside_into(ref, block, value):
        high, low = halves(value)
        for part, piece in enumerate((high, low, high)):
            ref[:, at(3 * block + part)] = piece

    def early_lead():
        coupling_copies[count - 1].wait()
        for k in range(count - 1):
            beside_into(x_ref, k, m_ref[at(count - 1), at(k)])
        yield
        depth = slice(0, 3 * (size - BLK))
        for k in range(0, count, 2):
            wide = slice(k * BLK, (k + 2) * BLK)
            value = coupling_ref[size - BLK :, wide] + dot_bf16(x_ref[:, depth], c_ref[depth, wide])
            stack(last_ref, wide, value)
            yield

    def project(i, left):
        depth = slice(0, 3 * (i + 1) * BLK)
        if i + 1 < count:
            for k in range(i):
                beside_into(x_ref, k, m_ref[at(i), at(k)])
            x_ref[:, 3 * i * BLK : 3 * (i + 1) * BLK] = left
            yield
        for k in range(0, count, 2):
            wide = slice(k * BLK, (k + 2) * BLK)
            if i + 1 == count:
                lead = dot_bf16(left, last_ref[:, wide])
            else:
                lead = dot_bf16(x_ref[:, depth], c_ref[depth, wide])
            for q in range(2):
                keep = inv_mask[i, row * count + k + q].astype(F32)
                beside_into(lead_stack, k + q, lead[:, q * BLK : (q + 1) * BLK] * keep)
            yield
        mine = m_ref[at(i), pl.ds(pl.multiple_of(row // 2 * BLK, BLK), BLK)]
        keep = inv_mask[i, inv_mask.shape[1] - count + row // 2]
        mine = beside(jnp.where((keep != 0) & (row // 2 <= i), mine, 0.0))
        half = BLK // 2
        for n in range(0, k_ref.shape[1], 2 * BLK):
            wide = slice(n, n + 2 * BLK)
            total = dot_bf16(mine, t_ref[:, wide]) - dot_bf16(lead_stack[...], k_ref[:, wide])
            kept_ref[i, :, wide] = jnp.where(core == 0, total[:half], total[half:])
            sent_ref[i, :, wide] = jnp.where(core == 0, total[half:], total[:half])
            yield

    fillers = [arrive(), prepare_row(0), pause(6), prepare(), split_coupling(0)]
    for j in range(count):
        rows = [m_ref[j * BLK + 8 * g : j * BLK + 8 * g + 8, at(j)] for g in range(16)]
        for step in factor_panels(rows, sub, lane, lines_ref):
            for _ in range(4):
                while fillers:
                    try:
                        next(fillers[0])
                        break
                    except StopIteration:
                        fillers.pop(0)
        while fillers:
            for _ in fillers.pop(0):
                pass
        p = jnp.concatenate([jnp.where(lane <= sub + 8 * g, rows[g], 0.0) for g in range(16)], axis=0)
        right = right_refs[j % 2]
        left = beside(p)
        m_ref[at(j), at(j)] = p
        stack(right, at(j), p)
        if j + 1 < count:
            u = dot_bf16(left, before_ref[:, at(j + 1)])
            m_ref[at(j), at(j + 1)] = u
            stack(right, at(j + 1), u)
            left_ref[j + 1] = beside(u.T)
            eliminate(j, j + 1, [at(j + 1)])
        spans = [slice(0, j * BLK)] if j > 0 else []
        if j + 2 < count:
            spans.append(slice((j + 2) * BLK, size))
        for span in spans:
            u = dot_bf16(left, before_ref[:, span])
            m_ref[at(j), span] = u
            stack(right, span, u)
        fillers = []
        if j + 1 < count:
            fillers += [trailing(j, j + 1, True), prepare_row(j + 1)]
            if j + 2 < count:
                fillers.append(split_coupling(j + 1))
            else:
                fillers.append(early_lead())
        fillers += [trailing(j, i, False) for i in range(j + 2, count)] + [project(j, left)]
    while fillers:
        for _ in fillers.pop(0):
            pass


def projected_part(place, inv_mask, ks_mask, mine, other, coupling, ks_lead, ks_tail):
    size = coupling.shape[0]
    lead, width = ks_lead.shape
    vmem = pl.BlockSpec(memory_space=pltpu.VMEM)
    smem = pl.BlockSpec(memory_space=pltpu.SMEM)
    hbm = pl.BlockSpec(memory_space=pl.ANY)
    return pl.pallas_call(
        kernel,
        out_shape=[jax.ShapeDtypeStruct((size // BLK, BLK // 2, width), F32)] * 2,
        in_specs=[smem, smem, smem, hbm, hbm, hbm, hbm, hbm],
        out_specs=[vmem, vmem],
        scratch_shapes=[
            pltpu.VMEM((size, size), F32),
            pltpu.VMEM(coupling.shape, F32),
            pltpu.VMEM(ks_lead.shape, F32),
            pltpu.VMEM(ks_tail.shape, F32),
            pltpu.VMEM((3 * size, coupling.shape[1]), BF16),
            pltpu.VMEM((3 * lead, width), BF16),
            pltpu.VMEM((3 * BLK, width), BF16),
            pltpu.VMEM((BLK, 3 * size), BF16),
            pltpu.VMEM((BLK, 3 * lead), BF16),
            pltpu.VMEM((3 * BLK, size), BF16),
            pltpu.VMEM((3 * BLK, size), BF16),
            pltpu.VMEM((3 * BLK, size), BF16),
            pltpu.VMEM((size // BLK, BLK, 3 * BLK), BF16),
            pltpu.VMEM((5, 3 * BLK, BLK), BF16),
            pltpu.VMEM((3 * BLK, size), BF16),
            pltpu.SemaphoreType.DMA((17,)),
            pltpu.SemaphoreType.DMA((28,)),
        ],
        compiler_params=pltpu.CompilerParams(vmem_limit_bytes=48 * 1024 * 1024),
        name="project",
    )(place, inv_mask, ks_mask, mine, other, coupling, ks_lead, ks_tail)


def pieces_first(where_ref, kept, got, z_kept, z_sent, x_own, *x_sent):
    x, z = where_ref[3], where_ref[4]
    half = kept.shape[-1] // 2
    lo, hi = slice(0, half), slice(half, 2 * half)
    for i in range(4):
        z_kept[i] = kept[2 * i + z, :, lo] + got[2 * i + z, :, lo]
        z_sent[i] = kept[2 * i + 1 - z, :, lo] + got[2 * i + 1 - z, :, lo]
    for k, ref in enumerate((x_own, *x_sent)):
        to = lax.rem(x + k, 4)
        for i in range(2):
            ref[i] = kept[2 * to + i, :, hi] + got[2 * to + i, :, hi]


def pieces_second(where_ref, z_kept, z_got, x_own, x1, x2, x3, y_own, y1, y2, y3, v_kept, v_sent):
    x, z = where_ref[3], where_ref[4]
    for k, ref in enumerate((y_own, y1, y2, y3)):
        to = lax.rem(x + k, 4)
        ref[...] = z_kept[to] + z_got[to]
    for ref, i in ((v_kept, z), (v_sent, 1 - z)):
        ref[...] = (x_own[i] + x1[i]) + (x2[i] + x3[i])


def pieces_third(y_own, y1, y2, y3, v_kept, v_got, out):
    half = out.shape[-1] // 2
    out[:, :half] = (y_own[...] + y1[...]) + (y2[...] + y3[...])
    out[:, half:] = v_kept[...] + v_got[...]


def summed(where, kept, sent):
    vmem = pl.BlockSpec(memory_space=pltpu.VMEM)
    smem = pl.BlockSpec(memory_space=pltpu.SMEM)
    swap = [(0, 1), (1, 0)]
    rows, half = kept.shape[1], kept.shape[2] // 2

    def shape(*lead):
        return jax.ShapeDtypeStruct((*lead, rows, half), F32)

    def turned(parts):
        return [
            lax.ppermute(part, "row_0", [(s, (s + k) % 4) for s in range(4)])
            for k, part in zip((1, 2, 3), parts)
        ]

    got = lax.ppermute(sent, "row_2", swap)
    z_kept, z_sent, x_own, *x_sent = pl.pallas_call(
        pieces_first,
        out_shape=[shape(4), shape(4)] + [shape(2)] * 4,
        in_specs=[smem, vmem, vmem],
        out_specs=[vmem] * 6,
        compiler_params=pltpu.CompilerParams(vmem_limit_bytes=4 * 1024 * 1024),
        name="pieces_first",
    )(where, kept, got)
    z_got = lax.ppermute(z_sent, "row_1", swap)
    x_got = turned(x_sent)
    y_own, y1, y2, y3, v_kept, v_sent = pl.pallas_call(
        pieces_second,
        out_shape=[shape()] * 6,
        in_specs=[smem] + [vmem] * 6,
        out_specs=[vmem] * 6,
        compiler_params=pltpu.CompilerParams(vmem_limit_bytes=4 * 1024 * 1024),
        name="pieces_second",
    )(where, z_kept, z_got, x_own, *x_got)
    v_got = lax.ppermute(v_sent, "row_1", swap)
    y_got = turned((y1, y2, y3))
    return pl.pallas_call(
        pieces_third,
        out_shape=jax.ShapeDtypeStruct((rows, 2 * half), F32),
        in_specs=[vmem] * 6,
        out_specs=vmem,
        compiler_params=pltpu.CompilerParams(vmem_limit_bytes=4 * 1024 * 1024),
        name="pieces_third",
    )(y_own, *y_got, v_kept, v_got)


def per_device(schur_tail, coupling, ks_lead, ks_tail, inv_mask, ks_mask):
    row_index = lax.axis_index(ROW)
    col_index = lax.axis_index(COL)
    core_index = lax.axis_index("row_2")
    twice = jnp.concatenate([schur_tail, schur_tail[:, : SENT * BLK - BLK]], axis=1)
    strip = lax.dynamic_slice_in_dim(twice, row_index // 2 * BLK, SENT * BLK, 1)
    chips = 1
    for axis in CHIPS:
        chips *= lax.axis_size(axis)
    copies = jnp.broadcast_to(strip[None], (chips,) + strip.shape)
    mine = lax.all_to_all(copies, CHIPS, split_axis=0, concat_axis=0, tiled=True)
    mine = mine.reshape(-1, BLK // 2, SENT * BLK)
    other = lax.ppermute(mine, "row_2", [(0, 1), (1, 0)])
    place = jnp.stack(
        [row_index, col_index, core_index, lax.axis_index("row_0"), lax.axis_index("row_1")]
    ).astype(jnp.int32)
    kept, sent = projected_part(place, inv_mask, ks_mask, mine, other, coupling, ks_lead, ks_tail)
    return summed(place, kept, sent)


def solution(mesh):
    split = Mesh(mesh.devices.reshape(4, 2, 2, 4, 2), ROW_COL)
    return jax.shard_map(
        per_device,
        mesh=split,
        in_specs=(P(ROW_COL, None), P(None, ROW), P(ROW, COL), P(ROW, COL), P(), P()),
        out_specs=P(ROW, COL),
        check_vma=False,
    )
```

```python
import jax
import jax.numpy as jnp
from jax import lax
from jax.experimental import pallas as pl
from jax.experimental.pallas import tpu as pltpu
from jax.sharding import Mesh
from jax.sharding import PartitionSpec as P

BLK = 128
ROW = ("row_0", "row_1", "row_2")
COL = ("col_0", "col_1")
ROW_COL = ROW + COL
CHIPS = ("row_0", "row_1", "col_0", "col_1")
F32 = jnp.float32
BF16 = jnp.bfloat16
SENT = 5


def dot_bf16(a, b):
    return jnp.dot(a, b, preferred_element_type=F32)


def halves(x):
    high = x.astype(BF16)
    return high, (x - high.astype(F32)).astype(BF16)


def lane_copy(x, column):
    return jnp.take_along_axis(x, jnp.full((8, BLK), column, jnp.int32), axis=1)


def row_copy(x, row):
    return jnp.broadcast_to(x[row : row + 1, :], (8, BLK))


def factor_panels(rows, sub, lane, lines_ref):
    groups = len(rows)
    for t in range(0, groups, 2):
        first = 8 * t
        pivot = [[], []]
        for m in range(16):
            for y in range(2):
                pivot[y].append(lane_copy(rows[t + y], first + m))
        near = range(t + 2, min(groups, t + 6))
        far = range(t + 6, groups)
        below = {g: [] for g in near}
        for pair in range(0, len(near), 2):
            for m in range(16):
                for g in near[pair : pair + 2]:
                    below[g].append(lane_copy(rows[g], first + m))
        here = (lane >= first) & (lane < first + 16)
        full = [
            jnp.where(here, jnp.where(lane - first - 8 * y == sub, 1.0, 0.0), rows[t + y])
            for y in range(2)
        ]
        result = list(full)
        inverses = []
        for k in range(0, 16, 2):
            x, i = k // 8, k % 8
            a = row_copy(pivot[x][k], i)
            b = row_copy(pivot[x][k + 1], i)
            c = row_copy(pivot[x][k + 1], i + 1)
            det = a * c - b * b
            root = lax.rsqrt(det)
            q = root * root
            left = []
            for y in range(2):
                u, v = pivot[y][k], pivot[y][k + 1]
                u, v = u * c - v * b, v * a - u * b
                if y == x:
                    others = (sub < i) | (sub > i + 1)
                    u, v = jnp.where(others, u, 0.0), jnp.where(others, v, 0.0)
                left.append((u, v))
            for m in range(k + 2, min(k + 4, 16)):
                top, low = row_copy(pivot[x][m], i), row_copy(pivot[x][m], i + 1)
                for y in range(2):
                    pivot[y][m] = pivot[y][m] - (left[y][0] * top + left[y][1] * low) * q
            left = [(u * q, v * q) for u, v in left]
            for m in range(k + 4, 16):
                top, low = row_copy(pivot[x][m], i), row_copy(pivot[x][m], i + 1)
                for y in range(2):
                    pivot[y][m] = pivot[y][m] - (left[y][0] * top + left[y][1] * low)
            top, low = row_copy(full[x], i), row_copy(full[x], i + 1)
            for y in range(2):
                full[y] = full[y] - (left[y][0] * top + left[y][1] * low)
            root_a = lax.rsqrt(a)
            over_a = root_a * root_a
            root_c = lax.rsqrt(det * over_a)
            result[x] = jnp.where(
                sub == i,
                top * root_a,
                jnp.where(sub == i + 1, (low - b * over_a * top) * root_c, result[x]),
            )
            inverses.append((q * a, q * b, q * c))
        rows[t], rows[t + 1] = result
        if below:
            lines = []
            for k in range(0, 16, 2):
                qa, qb, qc = inverses[k // 2]
                top = row_copy(full[k // 8], k % 8)
                low = row_copy(full[k // 8], k % 8 + 1)
                lines += [qc * top - qb * low, qa * low - qb * top]

            for g in near:
                terms = [a * b for a, b in zip(below[g], lines)]
                while len(terms) > 1:
                    terms = [a + b for a, b in zip(terms[::2], terms[1::2])]
                rows[g] = jnp.where(here, 0.0, rows[g]) - terms[0]
        if far:
            tall = []
            for y in range(2):
                value = lines[8 * y]
                for i in range(1, 8):
                    value = jnp.where(sub == i, lines[8 * y + i], value)
                tall.append(value)
            high, low = halves(jnp.concatenate(tall, axis=0))
            for part, value in enumerate((high, high, low)):
                lines_ref[t // 2, part * BLK + first : part * BLK + first + 16, :] = value
            high, low = halves(jnp.concatenate([rows[g] for g in far], axis=0))
            update = dot_bf16(jnp.concatenate([high, low, high], axis=1), lines_ref[t // 2])
            for i, g in enumerate(far):
                rows[g] = jnp.where(here, 0.0, rows[g]) - update[8 * i : 8 * i + 8]
        yield


def at_ds(i):
    return pl.ds(i * BLK, BLK)


def kernel(
    where_ref, inv_mask, ks_mask, mine_ref, other_ref, coupling_hbm, lead_hbm, tail_hbm,
    kept_ref, sent_ref,
    m_ref, coupling_ref, lead_ref, tail_ref, c_ref, k_ref, t_ref, x_ref, lead_stack,
    before_ref, right_even, right_odd, left_ref, lines_ref, last_ref, sem,
):
    right_refs = (right_even, right_odd)
    size = m_ref.shape[0]
    count = size // BLK
    row, col, core = where_ref[0], where_ref[1], where_ref[2]
    lead_copies = [
        pltpu.make_async_copy(lead_hbm.at[at_ds(k), :], lead_ref.at[at_ds(k), :], sem.at[k])
        for k in range(count)
    ]
    coupling_copies = [
        pltpu.make_async_copy(
            coupling_hbm.at[at_ds(k), :], coupling_ref.at[at_ds(k), :], sem.at[count + k]
        )
        for k in range(count)
    ]
    tail_copy = pltpu.make_async_copy(tail_hbm, tail_ref, sem.at[2 * count])
    sub = lax.broadcasted_iota(jnp.int32, (8, BLK), 0)
    lane = lax.broadcasted_iota(jnp.int32, (8, BLK), 1)

    def at(i):
        return slice(i * BLK, (i + 1) * BLK)

    def place(b):
        for ref, part in ((mine_ref, core), (other_ref, 1 - core)):
            held = pl.ds(pl.multiple_of(b * BLK + part * 64, 64), 64)
            direct = min(SENT, count - b) * BLK
            m_ref[held, b * BLK : b * BLK + direct] = ref[b, :, :direct]
            for o in range(count - b, SENT - 1):
                m_ref[held, at(b + o - count)] = ref[b, :, at(o)]

    tail_copy.start()
    for k in range(count):
        lead_copies[k].start()
    for k in range(count):
        coupling_copies[k].start()
    lines_ref[...] = jnp.zeros(lines_ref.shape, BF16)
    place(0)

    def arrive():
        for b in range(SENT, count):
            place(b)
            yield
        for b in range(1, SENT):
            place(b)
            yield
        for b in range(SENT, count):
            for c in range(b - SENT + 1):
                m_ref[at(c), at(b)] = m_ref[at(b), at(c)].T
            yield

    def pause(steps):
        for _ in range(steps):
            yield

    def split_coupling(k):
        coupling_copies[k].wait()
        for half in range(2):
            wide = slice(half * size // 2, (half + 1) * size // 2)
            high, low = halves(coupling_ref[at(k), wide])
            for part, value in enumerate((high, high, low)):
                c_ref[at(3 * k + part), wide] = value
            yield

    def prepare():
        for k in range(count):
            lead_copies[k].wait()
            for n in range(lead_ref.shape[1] // BLK):
                keep = ks_mask[row * count + k, col * 4 + n].astype(F32)
                high, low = halves(lead_ref[at(k), at(n)] * keep)
                for part, value in enumerate((high, high, low)):
                    k_ref[at(3 * k + part), at(n)] = value
            yield
        tail_copy.wait()
        t_ref[...] = jnp.zeros(t_ref.shape, BF16)
        lead_blocks = ks_mask.shape[0] - count
        for n in range(lead_ref.shape[1] // BLK):
            keep = ks_mask[lead_blocks + row // 2, col * 4 + n].astype(F32)
            high, low = halves(tail_ref[:, at(n)] * keep)
            for part, value in enumerate((high, high, low)):
                t_ref[pl.ds(pl.multiple_of(part * BLK + core * 64, 64), 64), at(n)] = value
        yield

    def stack(ref, cols, value):
        high, low = halves(value)
        ref[0:BLK, cols] = high
        ref[BLK : 2 * BLK, cols] = high
        ref[2 * BLK :, cols] = low

    def beside(value):
        high, low = halves(value)
        return jnp.concatenate([high, low, high], axis=1)

    def eliminate(j, i, parts):
        right = right_refs[j % 2]
        left = left_ref[i]
        for cols in parts:
            start, stop = cols.start, cols.stop
            update = dot_bf16(left, right[:, cols])
            if start == j * BLK and stop == start + BLK:
                m_ref[at(i), cols] = -update
            else:
                m_ref[at(i), cols] -= update

    def prepare_row(j):
        if j > 0:
            stack(before_ref, slice(0, j * BLK), m_ref[at(j), : j * BLK])
            yield
        if j + 1 < count:
            stack(before_ref, slice((j + 1) * BLK, size), m_ref[at(j), (j + 1) * BLK :])
            yield

    def trailing(j, i, first):
        if not first:
            left_ref[i] = beside(m_ref[at(j), at(i)].T)
        parts = [slice(c * BLK, (c + 1) * BLK) for c in (j,)]
        if j > 0:
            parts.append(slice(0, j * BLK))
        start = (i + 1 if first else i) * BLK
        if start < size:
            parts.append(slice(start, size))
        for part in parts:
            eliminate(j, i, [part])
            yield

    def beside_into(ref, block, value):
        high, low = halves(value)
        for part, piece in enumerate((high, low, high)):
            ref[:, at(3 * block + part)] = piece

    def early_lead():
        coupling_copies[count - 1].wait()
        for k in range(count - 1):
            beside_into(x_ref, k, m_ref[at(count - 1), at(k)])
        yield
        depth = slice(0, 3 * (size - BLK))
        for k in range(0, count, 2):
            wide = slice(k * BLK, (k + 2) * BLK)
            value = coupling_ref[size - BLK :, wide] + dot_bf16(x_ref[:, depth], c_ref[depth, wide])
            stack(last_ref, wide, value)
            yield

    def project(i, left):
        depth = slice(0, 3 * (i + 1) * BLK)
        if i + 1 < count:
            for k in range(i):
                beside_into(x_ref, k, m_ref[at(i), at(k)])
            x_ref[:, 3 * i * BLK : 3 * (i + 1) * BLK] = left
            yield
        for k in range(0, count, 2):
            wide = slice(k * BLK, (k + 2) * BLK)
            if i + 1 == count:
                lead = dot_bf16(left, last_ref[:, wide])
            else:
                lead = dot_bf16(x_ref[:, depth], c_ref[depth, wide])
            for q in range(2):
                keep = inv_mask[i, row * count + k + q].astype(F32)
                beside_into(lead_stack, k + q, lead[:, q * BLK : (q + 1) * BLK] * keep)
            yield
        mine = m_ref[at(i), pl.ds(pl.multiple_of(row // 2 * BLK, BLK), BLK)]
        keep = inv_mask[i, inv_mask.shape[1] - count + row // 2]
        mine = beside(jnp.where((keep != 0) & (row // 2 <= i), mine, 0.0))
        half = BLK // 2
        for n in range(0, k_ref.shape[1], 2 * BLK):
            wide = slice(n, n + 2 * BLK)
            total = dot_bf16(mine, t_ref[:, wide]) - dot_bf16(lead_stack[...], k_ref[:, wide])
            kept_ref[i, :, wide] = jnp.where(core == 0, total[:half], total[half:])
            sent_ref[i, :, wide] = jnp.where(core == 0, total[half:], total[:half])
            yield

    fillers = [arrive(), prepare_row(0), pause(2), prepare(), split_coupling(0)]
    for j in range(count):
        rows = [m_ref[j * BLK + 8 * g : j * BLK + 8 * g + 8, at(j)] for g in range(16)]
        for step in factor_panels(rows, sub, lane, lines_ref):
            for _ in range(4):
                while fillers:
                    try:
                        next(fillers[0])
                        break
                    except StopIteration:
                        fillers.pop(0)
        while fillers:
            for _ in fillers.pop(0):
                pass
        p = jnp.concatenate([jnp.where(lane <= sub + 8 * g, rows[g], 0.0) for g in range(16)], axis=0)
        right = right_refs[j % 2]
        left = beside(p)
        m_ref[at(j), at(j)] = p
        stack(right, at(j), p)
        if j + 1 < count:
            u = dot_bf16(left, before_ref[:, at(j + 1)])
            m_ref[at(j), at(j + 1)] = u
            stack(right, at(j + 1), u)
            left_ref[j + 1] = beside(u.T)
            eliminate(j, j + 1, [at(j + 1)])
        spans = [slice(0, j * BLK)] if j > 0 else []
        if j + 2 < count:
            spans.append(slice((j + 2) * BLK, size))
        for span in spans:
            u = dot_bf16(left, before_ref[:, span])
            m_ref[at(j), span] = u
            stack(right, span, u)
        fillers = []
        if j + 1 < count:
            fillers += [trailing(j, j + 1, True), prepare_row(j + 1)]
            if j + 2 < count:
                fillers.append(split_coupling(j + 1))
            else:
                fillers.append(early_lead())
        fillers += [trailing(j, i, False) for i in range(j + 2, count)] + [project(j, left)]
    while fillers:
        for _ in fillers.pop(0):
            pass


def projected_part(place, inv_mask, ks_mask, mine, other, coupling, ks_lead, ks_tail):
    size = coupling.shape[0]
    lead, width = ks_lead.shape
    vmem = pl.BlockSpec(memory_space=pltpu.VMEM)
    smem = pl.BlockSpec(memory_space=pltpu.SMEM)
    hbm = pl.BlockSpec(memory_space=pl.ANY)
    return pl.pallas_call(
        kernel,
        out_shape=[jax.ShapeDtypeStruct((size // BLK, BLK // 2, width), F32)] * 2,
        in_specs=[smem, smem, smem, vmem, vmem, hbm, hbm, hbm],
        out_specs=[vmem, vmem],
        scratch_shapes=[
            pltpu.VMEM((size, size), F32),
            pltpu.VMEM(coupling.shape, F32),
            pltpu.VMEM(ks_lead.shape, F32),
            pltpu.VMEM(ks_tail.shape, F32),
            pltpu.VMEM((3 * size, coupling.shape[1]), BF16),
            pltpu.VMEM((3 * lead, width), BF16),
            pltpu.VMEM((3 * BLK, width), BF16),
            pltpu.VMEM((BLK, 3 * size), BF16),
            pltpu.VMEM((BLK, 3 * lead), BF16),
            pltpu.VMEM((3 * BLK, size), BF16),
            pltpu.VMEM((3 * BLK, size), BF16),
            pltpu.VMEM((3 * BLK, size), BF16),
            pltpu.VMEM((size // BLK, BLK, 3 * BLK), BF16),
            pltpu.VMEM((5, 3 * BLK, BLK), BF16),
            pltpu.VMEM((3 * BLK, size), BF16),
            pltpu.SemaphoreType.DMA((17,)),
        ],
        compiler_params=pltpu.CompilerParams(vmem_limit_bytes=48 * 1024 * 1024),
        name="project",
    )(place, inv_mask, ks_mask, mine, other, coupling, ks_lead, ks_tail)


def pieces_first(where_ref, kept, got, z_kept, z_sent, x_own, *x_sent):
    x, z = where_ref[3], where_ref[4]
    half = kept.shape[-1] // 2
    lo, hi = slice(0, half), slice(half, 2 * half)
    for i in range(4):
        z_kept[i] = kept[2 * i + z, :, lo] + got[2 * i + z, :, lo]
        z_sent[i] = kept[2 * i + 1 - z, :, lo] + got[2 * i + 1 - z, :, lo]
    for k, ref in enumerate((x_own, *x_sent)):
        to = lax.rem(x + k, 4)
        for i in range(2):
            ref[i] = kept[2 * to + i, :, hi] + got[2 * to + i, :, hi]


def pieces_second(where_ref, z_kept, z_got, x_own, x1, x2, x3, y_own, y1, y2, y3, v_kept, v_sent):
    x, z = where_ref[3], where_ref[4]
    for k, ref in enumerate((y_own, y1, y2, y3)):
        to = lax.rem(x + k, 4)
        ref[...] = z_kept[to] + z_got[to]
    for ref, i in ((v_kept, z), (v_sent, 1 - z)):
        ref[...] = (x_own[i] + x1[i]) + (x2[i] + x3[i])


def pieces_third(y_own, y1, y2, y3, v_kept, v_got, out):
    half = out.shape[-1] // 2
    out[:, :half] = (y_own[...] + y1[...]) + (y2[...] + y3[...])
    out[:, half:] = v_kept[...] + v_got[...]


def summed(where, kept, sent):
    vmem = pl.BlockSpec(memory_space=pltpu.VMEM)
    smem = pl.BlockSpec(memory_space=pltpu.SMEM)
    swap = [(0, 1), (1, 0)]
    rows, half = kept.shape[1], kept.shape[2] // 2

    def shape(*lead):
        return jax.ShapeDtypeStruct((*lead, rows, half), F32)

    def turned(parts):
        return [
            lax.ppermute(part, "row_0", [(s, (s + k) % 4) for s in range(4)])
            for k, part in zip((1, 2, 3), parts)
        ]

    got = lax.ppermute(sent, "row_2", swap)
    z_kept, z_sent, x_own, *x_sent = pl.pallas_call(
        pieces_first,
        out_shape=[shape(4), shape(4)] + [shape(2)] * 4,
        in_specs=[smem, vmem, vmem],
        out_specs=[vmem] * 6,
        compiler_params=pltpu.CompilerParams(vmem_limit_bytes=4 * 1024 * 1024),
        name="pieces_first",
    )(where, kept, got)
    z_got = lax.ppermute(z_sent, "row_1", swap)
    x_got = turned(x_sent)
    y_own, y1, y2, y3, v_kept, v_sent = pl.pallas_call(
        pieces_second,
        out_shape=[shape()] * 6,
        in_specs=[smem] + [vmem] * 6,
        out_specs=[vmem] * 6,
        compiler_params=pltpu.CompilerParams(vmem_limit_bytes=4 * 1024 * 1024),
        name="pieces_second",
    )(where, z_kept, z_got, x_own, *x_got)
    v_got = lax.ppermute(v_sent, "row_1", swap)
    y_got = turned((y1, y2, y3))
    return pl.pallas_call(
        pieces_third,
        out_shape=jax.ShapeDtypeStruct((rows, 2 * half), F32),
        in_specs=[vmem] * 6,
        out_specs=vmem,
        compiler_params=pltpu.CompilerParams(vmem_limit_bytes=4 * 1024 * 1024),
        name="pieces_third",
    )(y_own, *y_got, v_kept, v_got)


def per_device(schur_tail, coupling, ks_lead, ks_tail, inv_mask, ks_mask):
    row_index = lax.axis_index(ROW)
    col_index = lax.axis_index(COL)
    core_index = lax.axis_index("row_2")
    twice = jnp.concatenate([schur_tail, schur_tail[:, : SENT * BLK - BLK]], axis=1)
    strip = lax.dynamic_slice_in_dim(twice, row_index // 2 * BLK, SENT * BLK, 1)
    chips = 1
    for axis in CHIPS:
        chips *= lax.axis_size(axis)
    copies = jnp.broadcast_to(strip[None], (chips,) + strip.shape)
    mine = lax.all_to_all(copies, CHIPS, split_axis=0, concat_axis=0, tiled=True)
    mine = mine.reshape(-1, BLK // 2, SENT * BLK)
    other = lax.ppermute(mine, "row_2", [(0, 1), (1, 0)])
    place = jnp.stack(
        [row_index, col_index, core_index, lax.axis_index("row_0"), lax.axis_index("row_1")]
    ).astype(jnp.int32)
    kept, sent = projected_part(place, inv_mask, ks_mask, mine, other, coupling, ks_lead, ks_tail)
    return summed(place, kept, sent)


def solution(mesh):
    split = Mesh(mesh.devices.reshape(4, 2, 2, 4, 2), ROW_COL)
    return jax.shard_map(
        per_device,
        mesh=split,
        in_specs=(P(ROW_COL, None), P(None, ROW), P(ROW, COL), P(ROW, COL), P(), P()),
        out_specs=P(ROW, COL),
        check_vma=False,
    )
```
